32 devices in a mesh: wide: 8 (over y, x, core), narrow: 4 (over z).
Axes of the slice: x: 2, y: 2, z: 4, core: 2. Of those that a mesh axis runs over, the one named last changes fastest.
Arguments:
- measures: float32 [2, 48, 262144], P(None, 'narrow', 'wide'), may hold values from 0.1 to 10
- sku_brand: int32 [262144], P('wide'), may hold values from 0 to 8191, as said below
- sku_count: int32 [8], P('wide'), may hold values from 1024 to 32768, as said below
- brand_slot: int32 [8192], replicated, may hold values from 0 to 8191, as said below
- brand_category: int32 [8192], replicated, may hold values from 0 to 499
Outputs:
- brand_index: float32 [2, 48, 8192], P(None, 'narrow', 'wide')
- category_index: float32 [2, 48, 500], P(None, 'narrow')
The draws below stay inside these ranges and needn't reach their ends.
Inputs may be any that keep to these rules, and one draw needn't show every extreme that they name: `sku_count`: the largest count is 32768 in every draw; the others are skewed below it. brand_slot is a permutation; columns k * 1024 to (k + 1) * 1024 - 1 form the k-th owner block. `sku_brand`: in every tile, slots o * 128 to (o + 1) * 128 - 1 name 128 distinct brands whose columns lie in owner block o, for every owner block o; every later slot of the tile names one of these brands; every brand is named by some live SKU.
All inputs are finite; a program needn't handle non-finite values.
Results may differ from the reference program's by a relative error of at most 0.002.
Values sent between devices are 32-bit elements; how exact they have to be, the bound alone decides.
A program may use at most 64 MiB of HBM per device.

```python
import math
import jax
import jax.numpy as jnp

WEEKS = 48
KINDS = 2
CATS = 500
CAP = 128
SKU_DEV = 32768
BR_DEV = 1024
SKUS = 262144
BRANDS = 8192
N_WIDE = 8


def slot_table_of(key):
    return jax.random.permutation(jax.random.fold_in(key, 11), BRANDS).astype(jnp.int32)


def draw_brand_slot(key, part):
    return slot_table_of(key)


def draw_sku_brand(key, part):
    slot_table = slot_table_of(key)
    inverse = jnp.zeros((BRANDS,), jnp.int32).at[slot_table].set(jnp.arange(BRANDS, dtype=jnp.int32))
    owner_keys = jax.random.split(jax.random.fold_in(key, 12), N_WIDE)
    owner_orders = jax.vmap(lambda subkey: jax.random.permutation(subkey, BR_DEV))(owner_keys).astype(jnp.int32)
    tile_ids = jnp.arange(N_WIDE, dtype=jnp.int32)[:, None]
    within = jnp.arange(CAP, dtype=jnp.int32)[None, :]
    positions = (tile_ids * CAP + within) % BR_DEV
    chosen = owner_orders[:, positions].transpose(1, 0, 2)
    columns = jnp.arange(N_WIDE, dtype=jnp.int32)[None, :, None] * BR_DEV + chosen
    first_brands = inverse[columns].reshape(N_WIDE, N_WIDE * CAP)
    filler = jax.random.randint(jax.random.fold_in(key, 13), (N_WIDE, SKU_DEV - N_WIDE * CAP), 0, N_WIDE * CAP)
    later_brands = jnp.take_along_axis(first_brands, filler.astype(jnp.int32), axis=1)
    return jnp.concatenate([first_brands, later_brands], axis=1).reshape(-1).astype(jnp.int32)


def draw_sku_count(key, part):
    floor_count = N_WIDE * CAP
    uniform_bits = jax.random.randint(jax.random.fold_in(key, 21), (N_WIDE,), 0, 1024).astype(jnp.int32)
    counts = floor_count + (SKU_DEV - floor_count) * (uniform_bits * uniform_bits // 1024) // 1024
    fullest = jax.random.randint(jax.random.fold_in(key, 22), (), 0, N_WIDE)
    counts = jnp.where(jnp.arange(N_WIDE, dtype=jnp.int32) == fullest, SKU_DEV, counts)
    return counts.astype(jnp.int32)


def with_ends(values, key, smallest, high):
    dims = values.shape
    place = [jax.random.randint(jax.random.fold_in(key, axis), (), 0, dims[axis]) for axis in range(len(dims))]
    values = values.at[tuple(place)].set(smallest)
    longest = dims.index(max(dims))
    place[longest] = (place[longest] + 1) % dims[longest]
    return values.at[tuple(place)].set(high)


def steps_of(key, extent, shards, least, largest):
    factor_of = 1.0
    for dim, shards_of in shards:
        draws = jax.random.uniform(jax.random.fold_in(jax.random.fold_in(key, 6), dim), (shards_of,), jnp.float32, least / len(shards), largest / len(shards))
        factor_of = factor_of * jnp.repeat(jnp.exp(draws), extent[dim] // shards_of).reshape((-1,) + (1,) * (len(extent) - 1 - dim))
    return factor_of


def setup_inputs(seed: int = 0) -> dict:
    seeds = jax.random.split(jax.random.key(seed), 6)
    measures = jnp.clip(jnp.exp(math.log(10.0) - 4.6051702 * jax.random.uniform(seeds[0], (KINDS, WEEKS, SKUS), jnp.float32) ** steps_of(seeds[0], (KINDS, WEEKS, SKUS), ((1, 4), (2, 8)), -0.2, 0.2)), 0.1, 10.0)
    sku_brand = draw_sku_brand(jax.random.fold_in(seeds[5], 71), 0)
    sku_count = draw_sku_count(jax.random.fold_in(seeds[5], 71), 0)
    brand_slot = draw_brand_slot(jax.random.fold_in(seeds[5], 71), 0)
    brand_category = with_ends(jax.random.randint(seeds[4], (BRANDS,), 0, CATS), jax.random.fold_in(seeds[4], 1), 0, CATS - 1).astype(jnp.int32)
    return dict(measures=measures, sku_brand=sku_brand, sku_count=sku_count, brand_slot=brand_slot, brand_category=brand_category)


def reference(measures, sku_brand, sku_count, brand_slot, brand_category):
    kind_count = measures.shape[0]
    is_live = (jnp.arange(SKU_DEV, dtype=jnp.int32)[None, :] < sku_count[:, None]).reshape(-1)
    masked = jnp.where(is_live[None, :], measures.reshape(kind_count * WEEKS, SKUS), 0.0).T
    brand_sums = jax.ops.segment_sum(masked, sku_brand, num_segments=BRANDS)
    category_sums = jax.ops.segment_sum(brand_sums, brand_category, num_segments=CATS)
    category_size = jax.ops.segment_sum(jnp.ones((BRANDS,), jnp.float32), brand_category, num_segments=CATS)
    relative = brand_sums * category_size[brand_category][:, None] / category_sums[brand_category]
    slotted = jnp.zeros_like(relative).at[brand_slot].set(relative)
    by_kind = category_sums.T.reshape(kind_count, WEEKS, CATS)
    grand_sum = jnp.sum(by_kind, axis=(1, 2)) / WEEKS
    category_index = by_kind * CATS / grand_sum[:, None, None]
    brand_index = slotted.T.reshape(kind_count, WEEKS, BRANDS)
    return brand_index, category_index
```

```python
import functools

import jax
import jax.numpy as jnp
from jax import lax
from jax.experimental import pallas as pl
from jax.experimental.pallas import tpu as pltpu
from jax.sharding import PartitionSpec as P

CATS = 500
CAP = 128
LANES = 128
LOW = 256
CAT_BLOCKS = 4
CAT_PAD = CAT_BLOCKS * LANES
NT = (((1,), (1,)), ((), ()))
MESH = pl.DeviceIdType.MESH
F32 = jnp.float32
BF16 = jnp.bfloat16


def dot_nt(a, b):
    return lax.dot_general(a, b, NT, preferred_element_type=F32)


def rows_of(shape):
    return lax.broadcasted_iota(jnp.int32, shape, 0)


def lanes_of(shape):
    return lax.broadcasted_iota(jnp.int32, shape, 1)


def split_two(x):
    high = x.astype(BF16).astype(F32)
    return jnp.concatenate([high, x - high], axis=0).astype(BF16)


def gather_lanes(row, index):
    table = jnp.broadcast_to(row, index.shape)
    return jnp.take_along_axis(table, index, axis=1, mode="promise_in_bounds")


def one_hot_rows(index, height):
    ids = rows_of((height, LANES))
    parts = [
        jnp.where(ids == index[i : i + 1, :], 1.0, 0.0).astype(BF16) for i in range(index.shape[0])
    ]
    return jnp.concatenate(parts, axis=1)


def local_kernel(
    n, owned, count_ref, brand_ref, list_ref, slot_ref, cat_ref, meas_ref, msg_ref, table, acc
):
    step = pl.program_id(0)
    kinds, weeks, block = meas_ref.shape
    rows = kinds * weeks
    table_rows = slot_ref.shape[0]
    half = table_rows // 2
    highs = n * CAP // LOW
    chunks = block // LANES

    @pl.when(step == 0)
    def _():
        listed = list_ref[...]
        ids = rows_of((table_rows, LANES))
        lane = lanes_of((table_rows, LANES))
        low_parts, high_parts = [], []
        for i in range(n):
            same = ids == (listed[i : i + 1, :] >> 7)
            position = i * CAP + lane
            low_parts.append(jnp.where(same, (position & 255).astype(F32), 0.0).astype(BF16))
            high_parts.append(jnp.where(same, (position >> 8).astype(F32), 0.0).astype(BF16))
        left = jnp.concatenate(
            [jnp.concatenate(low_parts, axis=1), jnp.concatenate(high_parts, axis=1)], axis=0
        )
        both = dot_nt(left, one_hot_rows(listed & 127, LANES))
        positions = (both[:table_rows] + 256.0 * both[table_rows:]).astype(jnp.int32)
        table[...] = positions[:half] | (positions[half:] << 16)
        acc[...] = jnp.zeros_like(acc)

    brands = brand_ref[...]
    high_bits, low_bits = brands >> 7, brands & 127
    group = high_bits & (half - 1)
    found = jnp.zeros_like(brands)
    for q in range(half):
        found = jnp.where(group == q, gather_lanes(table[q : q + 1, :], low_bits), found)
    position = jnp.where(high_bits >= half, found >> 16, found & 0xFFFF)
    slot = step * block + rows_of(brands.shape) * LANES + lanes_of(brands.shape)
    position = jnp.where(slot < count_ref[0], position, -1)
    low, high = position & (LOW - 1), position >> 8

    values = split_two(jnp.concatenate([meas_ref[k] for k in range(kinds)], axis=0))
    masked = []
    for i in range(chunks):
        part = values[:, i * LANES : (i + 1) * LANES]
        pieces = []
        for h in range(highs):
            mask = jnp.where(high[i : i + 1, :] == h, 1.0, 0.0)
            mask = jnp.broadcast_to(mask, part.shape).astype(BF16)
            pieces.append(part * mask)
        masked.append(jnp.concatenate(pieces, axis=0))
    acc[...] += dot_nt(jnp.concatenate(masked, axis=1), one_hot_rows(low, LOW))

    @pl.when(step == pl.num_programs(0) - 1)
    def _():
        sums = []
        for h in range(highs):
            at = h * 2 * rows
            sums.append(acc[at : at + rows] + acc[at + rows : at + 2 * rows])
        sums = jnp.concatenate(sums, axis=1)
        listed = list_ref[...]
        high_bits, low_bits = listed >> 7, listed & 127
        columns = jnp.zeros_like(listed)
        cats = jnp.zeros_like(listed)
        for q in range(table_rows):
            here = high_bits == q
            columns = jnp.where(here, gather_lanes(slot_ref[q : q + 1, :], low_bits), columns)
            cats = jnp.where(here, gather_lanes(cat_ref[q : q + 1, :], low_bits), cats)
        by_cat = dot_nt(split_two(sums), one_hot_rows(cats, CAT_PAD))
        by_cat = by_cat[:rows] + by_cat[rows:]
        me = lax.axis_index("wide")
        share = table_rows // n
        my_cats = cat_ref[pl.ds(pl.multiple_of(me * share, share), share), :]
        sizes = dot_nt(jnp.ones((8, share * LANES), BF16), one_hot_rows(my_cats, CAT_PAD))
        per_row = jnp.sum(sums, axis=1, keepdims=True)
        columns = lax.rem(columns, owned).astype(F32)
        cats = cats.astype(F32)
        ids = rows_of((8, LANES))
        notes = jnp.where(ids == 2, 1.0, 0.0)
        for k in range(kinds):
            inside = (rows_of((rows, 1)) // weeks) == k
            total = jnp.sum(jnp.where(inside, per_row, 0.0), axis=0, keepdims=True)
            notes = jnp.where(ids == 3 + k, jnp.broadcast_to(total, (8, LANES)), notes)
        for w in range(n):
            at = (w // (n // CAT_BLOCKS)) * LANES
            msg_ref[w, :rows, :] = sums[:, w * LANES : (w + 1) * LANES]
            msg_ref[w, rows : rows + 8, :] = jnp.where(
                ids == 0, columns[w : w + 1, :], jnp.where(ids == 1, cats[w : w + 1, :], notes)
            )
            msg_ref[w, rows + 8 : 2 * rows + 8, :] = by_cat[:, at : at + LANES]
            msg_ref[w, 2 * rows + 8 :, :] = sizes[:, at : at + LANES]


def share_kernel(
    n, m, kinds, weeks, msg_ref, brand_ref, category_ref,
    arrived, blocks, total, totals, send1, recv1, send2, recv2, send3, recv3,
):
    rows = kinds * weeks
    owned = brand_ref.shape[2]
    me, z = lax.axis_index("wide"), lax.axis_index("narrow")
    group = n // CAT_BLOCKS
    block, sub = me // group, lax.rem(me, group)

    barrier = pltpu.get_barrier_semaphore()
    for d in range(1, n):
        pl.semaphore_signal(
            barrier, inc=1, device_id=(lax.rem(me + d, n), z), device_id_type=MESH
        )
    for e in range(1, m):
        pl.semaphore_signal(
            barrier, inc=1, device_id=(me, lax.rem(z + e, m)), device_id_type=MESH
        )
    pl.semaphore_wait(barrier, n + m - 2)

    first = []
    for d in range(1, n):
        peer = lax.rem(me + d, n)
        copy = pltpu.make_async_remote_copy(
            src_ref=msg_ref.at[peer],
            dst_ref=arrived.at[d],
            send_sem=send1.at[d],
            recv_sem=recv1.at[d],
            device_id=(peer, z),
            device_id_type=MESH,
        )
        copy.start()
        first.append(copy)
    arrived[0] = msg_ref[me]
    for copy in first:
        copy.wait()

    split = rows + 8
    reduced = arrived[0, split:, :]
    notes = arrived[0, rows:split, :]
    for d in range(1, n):
        reduced = reduced + arrived[d, split:, :]
        notes = notes + arrived[d, rows:split, :]
    blocks[block] = reduced
    total[...] = notes
    second = []
    for e in range(1, CAT_BLOCKS):
        peer = lax.rem(block + e, CAT_BLOCKS) * group + sub
        copy = pltpu.make_async_remote_copy(
            src_ref=blocks.at[block],
            dst_ref=blocks.at[block],
            send_sem=send2.at[e],
            recv_sem=recv2.at[e],
            device_id=(peer, z),
            device_id_type=MESH,
        )
        copy.start()
        second.append(copy)
    for e in range(1, m):
        copy = pltpu.make_async_remote_copy(
            src_ref=total,
            dst_ref=totals.at[e],
            send_sem=send3.at[e],
            recv_sem=recv3.at[e],
            device_id=(me, lax.rem(z + e, m)),
            device_id_type=MESH,
        )
        copy.start()
        second.append(copy)

    entries = jnp.concatenate([arrived[d, :split, :] for d in range(n)], axis=1)
    ids = rows_of((owned, LANES)).astype(F32)
    placing = jnp.concatenate(
        [
            jnp.where(ids == arrived[d, rows : rows + 1, :], 1.0, 0.0).astype(BF16)
            for d in range(n)
        ],
        axis=1,
    )
    placed = dot_nt(split_two(entries), placing)
    placed = placed[:split] + placed[split:]
    my_cat = placed[rows + 1 : rows + 2, :] / placed[rows + 2 : rows + 3, :]
    cat_ids = rows_of((CAT_PAD, owned)).astype(F32)
    member = jnp.where(jnp.abs(my_cat - cat_ids) < 0.5, 1.0, 0.0).astype(BF16)

    for copy in second:
        copy.wait()
    every = jnp.concatenate([blocks[j] for j in range(CAT_BLOCKS)], axis=1)
    sums, sizes = every[:rows], every[rows : rows + 1]
    ratio = jnp.where(sums > 0.0, sizes / sums, 0.0)
    spread = jnp.dot(split_two(ratio), member, preferred_element_type=F32)
    relative = placed[:rows] * (spread[:rows] + spread[rows:])
    grand = total[...]
    for e in range(1, m):
        grand = grand + totals[e]
    for k in range(kinds):
        at = k * weeks
        brand_ref[k] = relative[at : at + weeks]
        scale = (CATS * weeks * m) / grand[3 + k : 4 + k, :1]
        category_ref[k] = (sums[at : at + weeks] * scale)[:, :CATS]


def body(n, m, measures, sku_brand, sku_count, brand_slot, brand_category):
    kinds, weeks, tile = measures.shape
    brand_total = brand_slot.shape[0]
    owned = brand_total // n
    rows = kinds * weeks
    table_rows = brand_total // LANES
    block = min(4096, tile)
    height = 2 * rows + 16
    brands = sku_brand.reshape(-1, LANES)
    whole = lambda shape: pl.BlockSpec(shape, lambda s: (0,) * len(shape))
    msg = pl.pallas_call(
        functools.partial(local_kernel, n, owned),
        grid=(tile // block,),
        out_shape=jax.ShapeDtypeStruct((n, height, LANES), F32),
        in_specs=[
            pl.BlockSpec(memory_space=pltpu.SMEM),
            pl.BlockSpec((block // LANES, LANES), lambda s: (s, 0)),
            whole((n, LANES)),
            whole((table_rows, LANES)),
            whole((table_rows, LANES)),
            pl.BlockSpec((kinds, weeks, block), lambda s: (0, 0, s)),
        ],
        out_specs=whole((n, height, LANES)),
        scratch_shapes=[
            pltpu.VMEM((table_rows // 2, LANES), jnp.int32),
            pltpu.VMEM((n * CAP // LOW * 2 * rows, LOW), F32),
        ],
        compiler_params=pltpu.CompilerParams(dimension_semantics=("arbitrary",)),
        name="tile_sums",
    )(
        sku_count,
        brands,
        brands,
        brand_slot.reshape(-1, LANES),
        brand_category.reshape(-1, LANES),
        measures,
    )
    dma = pltpu.SemaphoreType.DMA
    return pl.pallas_call(
        functools.partial(share_kernel, n, m, kinds, weeks),
        out_shape=(
            jax.ShapeDtypeStruct((kinds, weeks, owned), F32),
            jax.ShapeDtypeStruct((kinds, weeks, CATS), F32),
        ),
        in_specs=[pl.BlockSpec(memory_space=pltpu.VMEM)],
        out_specs=(
            pl.BlockSpec(memory_space=pltpu.VMEM),
            pl.BlockSpec(memory_space=pltpu.VMEM),
        ),
        scratch_shapes=[
            pltpu.VMEM((n, height, LANES), F32),
            pltpu.VMEM((CAT_BLOCKS, rows + 8, LANES), F32),
            pltpu.VMEM((8, LANES), F32),
            pltpu.VMEM((m, 8, LANES), F32),
            dma((n,)),
            dma((n,)),
            dma((CAT_BLOCKS,)),
            dma((CAT_BLOCKS,)),
            dma((m,)),
            dma((m,)),
        ],
        compiler_params=pltpu.CompilerParams(collective_id=0, has_side_effects=True),
        name="share_sums",
    )(msg)


def solution(mesh):
    n, m = mesh.shape["wide"], mesh.shape["narrow"]
    return jax.shard_map(
        functools.partial(body, n, m),
        mesh=mesh,
        in_specs=(P(None, "narrow", "wide"), P("wide"), P("wide"), P(), P()),
        out_specs=(P(None, "narrow", "wide"), P(None, "narrow", None)),
        check_vma=False,
    )
```

```python
import functools

import jax
import jax.numpy as jnp
from jax import lax
from jax.experimental import pallas as pl
from jax.experimental.pallas import tpu as pltpu
from jax.sharding import PartitionSpec as P

CATS = 500
CAP = 128
LANES = 128
CAT_BLOCKS = 4
CAT_PAD = CAT_BLOCKS * LANES
NT = (((1,), (1,)), ((), ()))
MESH = pl.DeviceIdType.MESH
F32 = jnp.float32
BF16 = jnp.bfloat16


def dot_nt(a, b):
    return lax.dot_general(a, b, NT, preferred_element_type=F32)


def rows_of(shape):
    return lax.broadcasted_iota(jnp.int32, shape, 0)


def lanes_of(shape):
    return lax.broadcasted_iota(jnp.int32, shape, 1)


def split_two(x):
    high = x.astype(BF16).astype(F32)
    return jnp.concatenate([high, x - high], axis=0).astype(BF16)


def gather_lanes(row, index):
    table = jnp.broadcast_to(row, index.shape)
    return jnp.take_along_axis(table, index, axis=1, mode="promise_in_bounds")


def one_hot_rows(index, height):
    ids = rows_of((height, LANES))
    parts = [
        jnp.where(ids == index[i : i + 1, :], 1.0, 0.0).astype(BF16) for i in range(index.shape[0])
    ]
    return jnp.concatenate(parts, axis=1)


def packed_row(row):
    return jnp.broadcast_to(row.astype(F32), (16, LANES)).astype(BF16)


def load_block(meas_ref, values, arrivals, step, per_block, start):
    weeks, _, kinds, _ = meas_ref.shape
    chunks = pl.ds(step * per_block, per_block)
    for w in range(weeks):
        copy = pltpu.make_async_copy(
            meas_ref.at[w, chunks],
            values.at[chunks, pl.ds(kinds * w, kinds)],
            arrivals.at[step, w],
        )
        if start:
            copy.start()
        else:
            copy.wait()


def local_sums(n, owned, count_ref, brand_ref, slot_ref, cat_ref, meas_ref, msg_ref, values, table, places, acc, arrivals):
    rows = values.shape[1]
    kinds = meas_ref.shape[2]
    table_rows = slot_ref.shape[0]
    half = table_rows // 2
    steps = arrivals.shape[0]
    per_block = values.shape[0] // steps

    listed = brand_ref[:n, :]
    ids = rows_of((table_rows, LANES))
    lane = lanes_of((table_rows, LANES))
    low_parts, high_parts = [], []
    for i in range(n):
        same = ids == (listed[i : i + 1, :] >> 7)
        low_parts.append(jnp.where(same, lane.astype(F32), 0.0).astype(BF16))
        high_parts.append(jnp.where(same, float(i), 0.0).astype(BF16))
    left = jnp.concatenate(
        [jnp.concatenate(low_parts, axis=1), jnp.concatenate(high_parts, axis=1)], axis=0
    )
    both = dot_nt(left, one_hot_rows(listed & 127, LANES))
    positions = (both[:table_rows] + float(CAP) * both[table_rows:]).astype(jnp.int32)
    table[...] = positions[:half] | (positions[half:] << 16)
    acc[...] = jnp.zeros_like(acc)

    def find(step, carry):
        here = pl.ds(pl.multiple_of(step * per_block, per_block), per_block)
        brands = brand_ref[here, :]
        high_bits, low_bits = brands >> 7, brands & 127
        group = high_bits & (half - 1)
        found = jnp.zeros_like(brands)
        for q in range(half):
            found = jnp.where(group == q, gather_lanes(table[q : q + 1, :], low_bits), found)
        position = jnp.where(high_bits >= half, found >> 16, found & 0xFFFF)
        slot = (step * per_block + rows_of(brands.shape)) * LANES + lanes_of(brands.shape)
        places[here, :] = jnp.where(slot < count_ref[0], position, -1)
        return carry

    lax.fori_loop(0, steps, find, 0)

    high_bits, low_bits = listed >> 7, listed & 127
    columns = jnp.zeros_like(listed)
    cats = jnp.zeros_like(listed)
    for q in range(table_rows):
        here = high_bits == q
        columns = jnp.where(here, gather_lanes(slot_ref[q : q + 1, :], low_bits), columns)
        cats = jnp.where(here, gather_lanes(cat_ref[q : q + 1, :], low_bits), cats)
    me = lax.axis_index("wide")
    share = table_rows // n
    my_cats = cat_ref[pl.ds(pl.multiple_of(me * share, share), share), :]
    sizes = dot_nt(jnp.ones((8, share * LANES), BF16), one_hot_rows(my_cats, CAT_PAD))
    by_list = one_hot_rows(cats, CAT_PAD)

    lane_ids = rows_of((LANES, LANES)).astype(F32).astype(BF16).reshape(LANES // 16, 16, LANES)
    one, zero = jnp.ones((), BF16), jnp.zeros((), BF16)

    def add(step, carry):
        load_block(meas_ref, values, arrivals, step, per_block, False)
        here = pl.multiple_of(step * per_block, per_block)
        position = places[pl.ds(here, per_block), :]
        low, high = position & (CAP - 1), position >> 7
        masked, hot = [], []
        for i in range(per_block):
            part = split_two(values[here + i]).reshape(2 * rows // 16, 16, LANES)
            owner = packed_row(high[i : i + 1, :])
            pieces = [
                jnp.where((owner == float(h))[None], part, zero).reshape(2 * rows, LANES)
                for h in range(n)
            ]
            masked.append(jnp.concatenate(pieces, axis=0))
            match = lane_ids == packed_row(low[i : i + 1, :])[None]
            hot.append(jnp.where(match, one, zero).reshape(LANES, LANES))
        acc[...] += dot_nt(jnp.concatenate(masked, axis=1), jnp.concatenate(hot, axis=1))
        return carry

    lax.fori_loop(0, steps, add, 0)

    sums = []
    for h in range(n):
        at = h * 2 * rows
        sums.append(acc[at : at + rows] + acc[at + rows : at + 2 * rows])
    sums = jnp.concatenate(sums, axis=1)
    by_cat = dot_nt(split_two(sums), by_list)
    by_cat = by_cat[:rows] + by_cat[rows:]
    per_row = jnp.sum(sums, axis=1, keepdims=True)
    columns = lax.rem(columns, owned).astype(F32)
    cats = cats.astype(F32)
    ids = rows_of((8, LANES))
    notes = jnp.where(ids == 2, 1.0, 0.0)
    for k in range(kinds):
        inside = lax.rem(rows_of((rows, 1)), kinds) == k
        total = jnp.sum(jnp.where(inside, per_row, 0.0), axis=0, keepdims=True)
        notes = jnp.where(ids == 3 + k, jnp.broadcast_to(total, (8, LANES)), notes)
    for w in range(n):
        at = (w // (n // CAT_BLOCKS)) * LANES
        msg_ref[w, 0, :rows, :] = by_cat[:, at : at + LANES]
        msg_ref[w, 0, rows:, :] = jnp.where(
            ids == 0, sizes[:, at : at + LANES], notes
        )
        msg_ref[w, 1, :rows, :] = sums[:, w * LANES : (w + 1) * LANES]
        msg_ref[w, 1, rows:, :] = jnp.where(
            ids == 0, columns[w : w + 1, :], jnp.where(ids == 1, cats[w : w + 1, :], notes)
        )


def rollup_kernel(
    n, m, owned, count_ref, brand_list_ref, slot_ref, cat_ref, meas_ref, brand_ref, category_ref,
    msg_ref, values, table, places, acc, arrivals,
    arrived, blocks, total, totals, send1, recv1, send2, recv2, send3, recv3,
):
    weeks, chunks, kinds, _ = meas_ref.shape
    rows = kinds * weeks
    steps = arrivals.shape[0]
    me, z = lax.axis_index("wide"), lax.axis_index("narrow")
    group = n // CAT_BLOCKS
    block, sub = me // group, lax.rem(me, group)

    barrier = pltpu.get_barrier_semaphore()
    for d in range(1, n):
        pl.semaphore_signal(
            barrier, inc=1, device_id=(lax.rem(me + d, n), z), device_id_type=MESH
        )
    for e in range(1, m):
        pl.semaphore_signal(
            barrier, inc=1, device_id=(me, lax.rem(z + e, m)), device_id_type=MESH
        )
    for step in range(steps):
        load_block(meas_ref, values, arrivals, step, chunks // steps, True)
    local_sums(
        n, owned, count_ref, brand_list_ref, slot_ref, cat_ref, meas_ref,
        msg_ref, values, table, places, acc, arrivals,
    )
    pl.semaphore_wait(barrier, n + m - 2)

    first = ([], [])
    for part in range(2):
        for d in range(1, n):
            peer = lax.rem(me + d, n)
            copy = pltpu.make_async_remote_copy(
                src_ref=msg_ref.at[peer, part],
                dst_ref=arrived.at[d, part],
                send_sem=send1.at[d, part],
                recv_sem=recv1.at[d, part],
                device_id=(peer, z),
                device_id_type=MESH,
            )
            copy.start()
            first[part].append(copy)
    reduced = msg_ref[me, 0]
    arrived[0, 1] = msg_ref[me, 1]
    for d in range(1, n):
        first[0][d - 1].wait()
        reduced = reduced + arrived[d, 0]
    blocks[block] = reduced
    total[...] = reduced[rows:]
    second = []
    for e in range(1, CAT_BLOCKS):
        peer = lax.rem(block + e, CAT_BLOCKS) * group + sub
        copy = pltpu.make_async_remote_copy(
            src_ref=blocks.at[block],
            dst_ref=blocks.at[block],
            send_sem=send2.at[e],
            recv_sem=recv2.at[e],
            device_id=(peer, z),
            device_id_type=MESH,
        )
        copy.start()
        second.append(copy)
    for e in range(1, m):
        copy = pltpu.make_async_remote_copy(
            src_ref=total,
            dst_ref=totals.at[e],
            send_sem=send3.at[e],
            recv_sem=recv3.at[e],
            device_id=(me, lax.rem(z + e, m)),
            device_id_type=MESH,
        )
        copy.start()
        second.append(copy)

    for copy in first[1]:
        copy.wait()
    split = rows + 8
    entries = jnp.concatenate([arrived[d, 1] for d in range(n)], axis=1)
    ids = rows_of((owned, LANES)).astype(F32)
    placing = jnp.concatenate(
        [
            jnp.where(ids == arrived[d, 1, rows : rows + 1, :], 1.0, 0.0).astype(BF16)
            for d in range(n)
        ],
        axis=1,
    )
    placed = dot_nt(split_two(entries), placing)
    placed = placed[:split] + placed[split:]
    my_cat = placed[rows + 1 : rows + 2, :] / placed[rows + 2 : rows + 3, :]
    cat_ids = rows_of((CAT_PAD, owned)).astype(F32)
    member = jnp.where(jnp.abs(my_cat - cat_ids) < 0.5, 1.0, 0.0).astype(BF16)

    for copy in second:
        copy.wait()
    every = jnp.concatenate([blocks[j] for j in range(CAT_BLOCKS)], axis=1)
    sums, sizes = every[:rows], every[rows : rows + 1]
    ratio = jnp.where(sums > 0.0, sizes / sums, 0.0)
    spread = jnp.dot(split_two(ratio), member, preferred_element_type=F32)
    relative = placed[:rows] * (spread[:rows] + spread[rows:])
    grand = total[...]
    for e in range(1, m):
        grand = grand + totals[e]
    scale = (CATS * weeks * m) / grand
    odd = lax.rem(rows_of((rows, 1)), kinds)
    row_scale = jnp.zeros((rows, 1), F32)
    for k in range(kinds):
        row_scale = jnp.where(odd == k, scale[3 + k : 4 + k, :1], row_scale)
    indices = sums * row_scale
    for w in range(weeks):
        at = kinds * w
        for c in range(owned // LANES):
            brand_ref[w, kinds * c : kinds * (c + 1), :] = relative[
                at : at + kinds, c * LANES : (c + 1) * LANES
            ]
        for c in range(CAT_BLOCKS):
            category_ref[w, kinds * c : kinds * (c + 1), :] = indices[
                at : at + kinds, c * LANES : (c + 1) * LANES
            ]


def body(n, m, measures, sku_brand, sku_count, brand_slot, brand_category):
    kinds, weeks, tile = measures.shape
    brand_total = brand_slot.shape[0]
    owned = brand_total // n
    rows = kinds * weeks
    table_rows = brand_total // LANES
    chunks = tile // LANES
    steps = chunks // 32
    by_chunk = measures.reshape(kinds, weeks, chunks, LANES).transpose(1, 2, 0, 3)
    dma = pltpu.SemaphoreType.DMA
    vmem = pl.BlockSpec(memory_space=pltpu.VMEM)
    brand_out, category_out = pl.pallas_call(
        functools.partial(rollup_kernel, n, m, owned),
        out_shape=(
            jax.ShapeDtypeStruct((weeks, kinds * owned // LANES, LANES), F32),
            jax.ShapeDtypeStruct((weeks, kinds * CAT_BLOCKS, LANES), F32),
        ),
        in_specs=[
            pl.BlockSpec(memory_space=pltpu.SMEM),
            vmem,
            vmem,
            vmem,
            pl.BlockSpec(memory_space=pl.ANY),
        ],
        out_specs=(vmem, vmem),
        scratch_shapes=[
            pltpu.VMEM((n, 2, rows + 8, LANES), F32),
            pltpu.VMEM((chunks, rows, LANES), F32),
            pltpu.VMEM((table_rows // 2, LANES), jnp.int32),
            pltpu.VMEM((chunks, LANES), jnp.int32),
            pltpu.VMEM((n * 2 * rows, LANES), F32),
            dma((steps, weeks)),
            pltpu.VMEM((n, 2, rows + 8, LANES), F32),
            pltpu.VMEM((CAT_BLOCKS, rows + 8, LANES), F32),
            pltpu.VMEM((8, LANES), F32),
            pltpu.VMEM((m, 8, LANES), F32),
            dma((n, 2)),
            dma((n, 2)),
            dma((CAT_BLOCKS,)),
            dma((CAT_BLOCKS,)),
            dma((m,)),
            dma((m,)),
        ],
        compiler_params=pltpu.CompilerParams(collective_id=0, has_side_effects=True),
        name="rollup",
    )(
        sku_count,
        sku_brand.reshape(-1, LANES),
        brand_slot.reshape(-1, LANES),
        brand_category.reshape(-1, LANES),
        by_chunk,
    )
    brand_index = brand_out.reshape(weeks, -1, kinds, LANES).transpose(2, 0, 1, 3)
    category_index = category_out.reshape(weeks, -1, kinds, LANES).transpose(2, 0, 1, 3)
    return (
        brand_index.reshape(kinds, weeks, owned),
        category_index.reshape(kinds, weeks, CAT_PAD)[:, :, :CATS],
    )


def solution(mesh):
    n, m = mesh.shape["wide"], mesh.shape["narrow"]
    return jax.shard_map(
        functools.partial(body, n, m),
        mesh=mesh,
        in_specs=(P(None, "narrow", "wide"), P("wide"), P("wide"), P(), P()),
        out_specs=(P(None, "narrow", "wide"), P(None, "narrow", None)),
        check_vma=False,
    )
```

```python
import functools

import jax
import jax.numpy as jnp
from jax import lax
from jax.experimental import pallas as pl
from jax.experimental.pallas import tpu as pltpu
from jax.sharding import PartitionSpec as P

CATS = 500
CAP = 128
LANES = 128
LOW = 256
CAT_BLOCKS = 4
CAT_PAD = CAT_BLOCKS * LANES
NT = (((1,), (1,)), ((), ()))
MESH = pl.DeviceIdType.MESH
F32 = jnp.float32
BF16 = jnp.bfloat16


def dot_nt(a, b):
    return lax.dot_general(a, b, NT, preferred_element_type=F32)


def rows_of(shape):
    return lax.broadcasted_iota(jnp.int32, shape, 0)


def lanes_of(shape):
    return lax.broadcasted_iota(jnp.int32, shape, 1)


def split_two(x):
    high = x.astype(BF16).astype(F32)
    return jnp.concatenate([high, x - high], axis=0).astype(BF16)


def gather_lanes(row, index):
    table = jnp.broadcast_to(row, index.shape)
    return jnp.take_along_axis(table, index, axis=1, mode="promise_in_bounds")


def packed_row(row):
    return jnp.broadcast_to(row.astype(F32), (16, LANES)).astype(BF16)


def one_hot_row(row, height):
    span = min(height, 256)
    ids = rows_of((span, LANES)).astype(F32).astype(BF16).reshape(span // 16, 16, LANES)
    one, zero = jnp.ones((), BF16), jnp.zeros((), BF16)
    parts = [
        jnp.where(ids == packed_row(row - base)[None], one, zero).reshape(span, LANES)
        for base in range(0, height, span)
    ]
    return jnp.concatenate(parts, axis=0)


def one_hot_rows(index, height):
    parts = [one_hot_row(index[i : i + 1, :], height) for i in range(index.shape[0])]
    return jnp.concatenate(parts, axis=1)


def load_block(meas_ref, values, arrivals, step, per_block, start):
    weeks, _, kinds, _ = meas_ref.shape
    chunks = pl.ds(step * per_block, per_block)
    for w in range(weeks):
        copy = pltpu.make_async_copy(
            meas_ref.at[w, chunks],
            values.at[chunks, pl.ds(kinds * w, kinds)],
            arrivals.at[step, w],
        )
        if start:
            copy.start()
        else:
            copy.wait()


def local_sums(n, owned, count_ref, brand_ref, slot_ref, cat_ref, meas_ref, msg_ref, values, table, places, acc, arrivals):
    rows = values.shape[1]
    kinds = meas_ref.shape[2]
    table_rows = slot_ref.shape[0]
    half = table_rows // 2
    steps = arrivals.shape[0]
    per_block = values.shape[0] // steps

    listed = brand_ref[:n, :]
    ids = rows_of((table_rows, LANES))
    lane = lanes_of((table_rows, LANES))
    low_parts, high_parts = [], []
    for i in range(n):
        same = ids == (listed[i : i + 1, :] >> 7)
        low_parts.append(jnp.where(same, lane.astype(F32), 0.0).astype(BF16))
        high_parts.append(jnp.where(same, float(i), 0.0).astype(BF16))
    left = jnp.concatenate(
        [jnp.concatenate(low_parts, axis=1), jnp.concatenate(high_parts, axis=1)], axis=0
    )
    both = dot_nt(left, one_hot_rows(listed & 127, LANES))
    positions = (both[:table_rows] + float(CAP) * both[table_rows:]).astype(jnp.int32)
    table[...] = positions[:half] | (positions[half:] << 16)
    acc[...] = jnp.zeros_like(acc)

    def find(step, carry):
        here = pl.ds(pl.multiple_of(step * per_block, per_block), per_block)
        brands = brand_ref[here, :]
        high_bits, low_bits = brands >> 7, brands & 127
        group = high_bits & (half - 1)
        found = jnp.zeros_like(brands)
        for q in range(half):
            found = jnp.where(group == q, gather_lanes(table[q : q + 1, :], low_bits), found)
        position = jnp.where(high_bits >= half, found >> 16, found & 0xFFFF)
        slot = (step * per_block + rows_of(brands.shape)) * LANES + lanes_of(brands.shape)
        places[here, :] = jnp.where(slot < count_ref[0], position, -1)
        return carry

    lax.fori_loop(0, steps, find, 0)

    high_bits, low_bits = listed >> 7, listed & 127
    columns = jnp.zeros_like(listed)
    cats = jnp.zeros_like(listed)
    for q in range(table_rows):
        here = high_bits == q
        columns = jnp.where(here, gather_lanes(slot_ref[q : q + 1, :], low_bits), columns)
        cats = jnp.where(here, gather_lanes(cat_ref[q : q + 1, :], low_bits), cats)
    me = lax.axis_index("wide")
    share = table_rows // n
    my_cats = cat_ref[pl.ds(pl.multiple_of(me * share, share), share), :]
    sizes = dot_nt(jnp.ones((8, share * LANES), BF16), one_hot_rows(my_cats, CAT_PAD))
    by_list = one_hot_rows(cats, CAT_PAD)

    highs = n * CAP // LOW
    lane_ids = [
        (lanes_of((LANES, LANES)) + at).astype(F32).astype(BF16) for at in range(0, LOW, LANES)
    ]
    one, zero = jnp.ones((), BF16), jnp.zeros((), BF16)

    def add(step, carry):
        load_block(meas_ref, values, arrivals, step, per_block, False)
        here = pl.multiple_of(step * per_block, per_block)
        position = places[pl.ds(here, per_block), :]
        low, high = position & (LOW - 1), position >> (LOW.bit_length() - 1)
        columns_of = jnp.transpose(low.astype(F32))
        masked, hot = [], []
        for i in range(per_block):
            part = split_two(values[here + i]).reshape(2 * rows // 16, 16, LANES)
            owner = packed_row(high[i : i + 1, :])
            pieces = [
                jnp.where((owner == float(h))[None], part, zero).reshape(2 * rows, LANES)
                for h in range(highs)
            ]
            masked.append(jnp.concatenate(pieces, axis=0))
            column = jnp.broadcast_to(columns_of[:, i : i + 1], (LANES, LANES)).astype(BF16)
            hot.append(
                jnp.concatenate([jnp.where(column == ids, one, zero) for ids in lane_ids], axis=1)
            )
        acc[...] += jnp.dot(
            jnp.concatenate(masked, axis=1),
            jnp.concatenate(hot, axis=0),
            preferred_element_type=F32,
        )
        return carry

    lax.fori_loop(0, steps, add, 0)

    sums = []
    for h in range(highs):
        at = h * 2 * rows
        sums.append(acc[at : at + rows] + acc[at + rows : at + 2 * rows])
    sums = jnp.concatenate(sums, axis=1)
    by_cat = dot_nt(split_two(sums), by_list)
    by_cat = by_cat[:rows] + by_cat[rows:]
    per_row = jnp.sum(sums, axis=1, keepdims=True)
    columns = lax.rem(columns, owned).astype(F32)
    cats = cats.astype(F32)
    ids = rows_of((8, LANES))
    notes = jnp.where(ids == 2, 1.0, 0.0)
    for k in range(kinds):
        inside = lax.rem(rows_of((rows, 1)), kinds) == k
        total = jnp.sum(jnp.where(inside, per_row, 0.0), axis=0, keepdims=True)
        notes = jnp.where(ids == 3 + k, jnp.broadcast_to(total, (8, LANES)), notes)
    for w in range(n):
        at = (w // (n // CAT_BLOCKS)) * LANES
        msg_ref[w, 0, :rows, :] = by_cat[:, at : at + LANES]
        msg_ref[w, 0, rows:, :] = jnp.where(
            ids == 0, sizes[:, at : at + LANES], notes
        )
        msg_ref[w, 1, :rows, :] = sums[:, w * LANES : (w + 1) * LANES]
        msg_ref[w, 1, rows:, :] = jnp.where(
            ids == 0, columns[w : w + 1, :], jnp.where(ids == 1, cats[w : w + 1, :], notes)
        )


def rollup_kernel(
    n, m, owned, count_ref, brand_list_ref, slot_ref, cat_ref, meas_ref, brand_ref, category_ref,
    msg_ref, values, table, places, acc, arrivals,
    arrived, blocks, total, totals, send1, recv1, send2, recv2, send3, recv3,
):
    weeks, chunks, kinds, _ = meas_ref.shape
    rows = kinds * weeks
    steps = arrivals.shape[0]
    me, z = lax.axis_index("wide"), lax.axis_index("narrow")
    group = n // CAT_BLOCKS
    block, sub = me // group, lax.rem(me, group)

    barrier = pltpu.get_barrier_semaphore()
    for d in range(1, n):
        pl.semaphore_signal(
            barrier, inc=1, device_id=(lax.rem(me + d, n), z), device_id_type=MESH
        )
    for e in range(1, m):
        pl.semaphore_signal(
            barrier, inc=1, device_id=(me, lax.rem(z + e, m)), device_id_type=MESH
        )
    for step in range(steps):
        load_block(meas_ref, values, arrivals, step, chunks // steps, True)
    local_sums(
        n, owned, count_ref, brand_list_ref, slot_ref, cat_ref, meas_ref,
        msg_ref, values, table, places, acc, arrivals,
    )
    pl.semaphore_wait(barrier, n + m - 2)

    first = ([], [])
    for part in range(2):
        for d in range(1, n):
            peer = lax.rem(me + d, n)
            copy = pltpu.make_async_remote_copy(
                src_ref=msg_ref.at[peer, part],
                dst_ref=arrived.at[d, part],
                send_sem=send1.at[d, part],
                recv_sem=recv1.at[d, part],
                device_id=(peer, z),
                device_id_type=MESH,
            )
            copy.start()
            first[part].append(copy)
    reduced = msg_ref[me, 0]
    arrived[0, 1] = msg_ref[me, 1]
    for d in range(1, n):
        first[0][d - 1].wait()
        reduced = reduced + arrived[d, 0]
    blocks[block] = reduced
    total[...] = reduced[rows:]
    second = []
    for e in range(1, CAT_BLOCKS):
        peer = lax.rem(block + e, CAT_BLOCKS) * group + sub
        copy = pltpu.make_async_remote_copy(
            src_ref=blocks.at[block],
            dst_ref=blocks.at[block],
            send_sem=send2.at[e],
            recv_sem=recv2.at[e],
            device_id=(peer, z),
            device_id_type=MESH,
        )
        copy.start()
        second.append(copy)
    for e in range(1, m):
        copy = pltpu.make_async_remote_copy(
            src_ref=total,
            dst_ref=totals.at[e],
            send_sem=send3.at[e],
            recv_sem=recv3.at[e],
            device_id=(me, lax.rem(z + e, m)),
            device_id_type=MESH,
        )
        copy.start()
        second.append(copy)

    for copy in first[1]:
        copy.wait()
    split = rows + 8
    entries = jnp.concatenate([arrived[d, 1] for d in range(n)], axis=1)
    placing = jnp.concatenate(
        [one_hot_row(arrived[d, 1, rows : rows + 1, :], owned) for d in range(n)], axis=1
    )
    placed = dot_nt(split_two(entries), placing)
    placed = placed[:split] + placed[split:]
    my_cat = placed[rows + 1 : rows + 2, :] / placed[rows + 2 : rows + 3, :]
    cat_ids = rows_of((CAT_PAD, owned)).astype(F32)
    member = jnp.where(jnp.abs(my_cat - cat_ids) < 0.5, 1.0, 0.0).astype(BF16)

    for copy in second:
        copy.wait()
    every = jnp.concatenate([blocks[j] for j in range(CAT_BLOCKS)], axis=1)
    sums, sizes = every[:rows], every[rows : rows + 1]
    ratio = jnp.where(sums > 0.0, sizes / sums, 0.0)
    spread = jnp.dot(split_two(ratio), member, preferred_element_type=F32)
    relative = placed[:rows] * (spread[:rows] + spread[rows:])
    grand = total[...]
    for e in range(1, m):
        grand = grand + totals[e]
    scale = (CATS * weeks * m) / grand
    odd = lax.rem(rows_of((rows, 1)), kinds)
    row_scale = jnp.zeros((rows, 1), F32)
    for k in range(kinds):
        row_scale = jnp.where(odd == k, scale[3 + k : 4 + k, :1], row_scale)
    indices = sums * row_scale
    for w in range(weeks):
        at = kinds * w
        for c in range(owned // LANES):
            brand_ref[w, kinds * c : kinds * (c + 1), :] = relative[
                at : at + kinds, c * LANES : (c + 1) * LANES
            ]
        for c in range(CAT_BLOCKS):
            category_ref[w, kinds * c : kinds * (c + 1), :] = indices[
                at : at + kinds, c * LANES : (c + 1) * LANES
            ]


def hand_out(brand_ref, category_ref, brand_out, category_out):
    brand_out[...] = brand_ref[...]
    category_out[...] = category_ref[...]


def body(n, m, measures, sku_brand, sku_count, brand_slot, brand_category):
    kinds, weeks, tile = measures.shape
    brand_total = brand_slot.shape[0]
    owned = brand_total // n
    rows = kinds * weeks
    table_rows = brand_total // LANES
    chunks = tile // LANES
    steps = chunks // 32
    by_chunk = measures.reshape(kinds, weeks, chunks, LANES).transpose(1, 2, 0, 3)
    dma = pltpu.SemaphoreType.DMA
    vmem = pl.BlockSpec(memory_space=pltpu.VMEM)
    brand_out, category_out = pl.pallas_call(
        functools.partial(rollup_kernel, n, m, owned),
        out_shape=(
            jax.ShapeDtypeStruct((weeks, kinds * owned // LANES, LANES), F32),
            jax.ShapeDtypeStruct((weeks, kinds * CAT_BLOCKS, LANES), F32),
        ),
        in_specs=[
            pl.BlockSpec(memory_space=pltpu.SMEM),
            vmem,
            vmem,
            vmem,
            pl.BlockSpec(memory_space=pl.ANY),
        ],
        out_specs=(vmem, vmem),
        scratch_shapes=[
            pltpu.VMEM((n, 2, rows + 8, LANES), F32),
            pltpu.VMEM((chunks, rows, LANES), F32),
            pltpu.VMEM((table_rows // 2, LANES), jnp.int32),
            pltpu.VMEM((chunks, LANES), jnp.int32),
            pltpu.VMEM((n * CAP // LOW * 2 * rows, LOW), F32),
            dma((steps, weeks)),
            pltpu.VMEM((n, 2, rows + 8, LANES), F32),
            pltpu.VMEM((CAT_BLOCKS, rows + 8, LANES), F32),
            pltpu.VMEM((8, LANES), F32),
            pltpu.VMEM((m, 8, LANES), F32),
            dma((n, 2)),
            dma((n, 2)),
            dma((CAT_BLOCKS,)),
            dma((CAT_BLOCKS,)),
            dma((m,)),
            dma((m,)),
        ],
        compiler_params=pltpu.CompilerParams(collective_id=0, has_side_effects=True),
        name="rollup",
    )(
        sku_count,
        sku_brand.reshape(-1, LANES),
        brand_slot.reshape(-1, LANES),
        brand_category.reshape(-1, LANES),
        by_chunk,
    )
    brand_out, category_out = pl.pallas_call(
        hand_out,
        out_shape=(
            jax.ShapeDtypeStruct(brand_out.shape, F32),
            jax.ShapeDtypeStruct(category_out.shape, F32),
        ),
        in_specs=[vmem, vmem],
        out_specs=(vmem, vmem),
        name="hand_out",
    )(brand_out, category_out)
    brand_index = brand_out.reshape(weeks, -1, kinds, LANES).transpose(2, 0, 1, 3)
    category_index = category_out.reshape(weeks, -1, kinds, LANES).transpose(2, 0, 1, 3)
    return (
        brand_index.reshape(kinds, weeks, owned),
        category_index.reshape(kinds, weeks, CAT_PAD)[:, :, :CATS],
    )


def solution(mesh):
    n, m = mesh.shape["wide"], mesh.shape["narrow"]
    return jax.shard_map(
        functools.partial(body, n, m),
        mesh=mesh,
        in_specs=(P(None, "narrow", "wide"), P("wide"), P("wide"), P(), P()),
        out_specs=(P(None, "narrow", "wide"), P(None, "narrow", None)),
        check_vma=False,
    )
```
